32 devices in a mesh: dp: 8 (over z, y), tensor: 4 (over x, core).
Axes of the slice: x: 2, y: 2, z: 4, core: 2. Of those that a mesh axis runs over, the one named last changes fastest.
Arguments:
- patches: bfloat16 [8192, 1280], P('dp', 'tensor'), may hold values from -60 to 60
- counts: int32 [16], replicated, may hold values from 0 to 512, as said below
- first_gain: float32 [1280], replicated, may hold values from 0.1 to 1.9
- first_shift: float32 [1280], replicated, may hold values from -3 to 3
- in_weight: bfloat16 [1280, 3, 1280], P(None, None, 'tensor'), may hold values from -0.15625 to 0.15625
- in_bias: float32 [3, 1280], P(None, 'tensor'), may hold values from -30 to 30
- out_weight: bfloat16 [1280, 1280], P(None, 'tensor'), may hold values from -0.15625 to 0.15625
- out_bias: float32 [1280], P('tensor'), may hold values from -3 to 3
- second_gain: float32 [1280], P('tensor'), may hold values from 0.1 to 1.9
- second_shift: float32 [1280], P('tensor'), may hold values from -3 to 3
- merger_weight: bfloat16 [4, 1280, 4096], P(None, 'tensor', 'dp'), may hold values from -0.078125 to 0.078125
- merger_bias: float32 [4096], replicated, may hold values from -4 to 4
Outputs:
- embeds: bfloat16 [2048, 4096], P(('dp', 'tensor'))
The draws below stay inside these ranges and needn't reach their ends.
Inputs may be any that keep to these rules, and one draw needn't show every extreme that they name: Entry 2 r + j is the patch count of slot j of data rank r, 0 for an empty slot; a rank's images fill its slots from slot 0; counts are multiples of 4; ranks 2 i and 2 i + 1 hold at most two images together, and in every draw some rank holds two.
All inputs are finite; a program needn't handle non-finite values.
Results may differ from the reference program's by a relative error of at most 0.0095.
Values may be sent and summed in bfloat16 or wider, within the bound.
No kernel may reach another device: no remote copies, remote signals or barrier semaphores. Data moves between devices by JAX's collectives and lax.ppermute only.
A program may use at most 128 MiB of HBM per device.

```python
import math
import jax
import jax.numpy as jnp
from jax import lax

D = 1280
HEADS = 16
LLMW = 4096
TILE = 512
IMAGE_SLOTS = 16
ROWS = 2048
N_TENSOR = 4


def draw_patches(key, part):
    first = jax.random.fold_in(jax.random.fold_in(key, 11), 0)
    base = jax.random.normal(first, (IMAGE_SLOTS * TILE, D), jnp.float32)
    return jnp.clip(base, -60.0, 60.0).astype(jnp.bfloat16)


def draw_in_bias(key, part):
    first = jax.random.fold_in(jax.random.fold_in(key, 23), 0)
    base = 0.5 * jax.random.normal(first, (3, D), jnp.float32)
    return jnp.clip(base, -30.0, 30.0)


def draw_counts(key, part):
    first, second, third = jax.random.split(jax.random.fold_in(key, 37), 3)
    pairs = IMAGE_SLOTS // 4
    pattern = jax.random.randint(first, (pairs,), 0, 6)
    forced = jax.random.randint(second, (), 0, 2)
    pattern = jnp.where(jnp.arange(pairs) == 0, forced, pattern)
    table_left = jnp.array([2, 0, 1, 1, 0, 0], jnp.int32)
    table_right = jnp.array([0, 2, 1, 0, 1, 0], jnp.int32)
    left = table_left[pattern]
    right = table_right[pattern]
    sizes = jax.random.randint(third, (pairs, 4), TILE // 8, TILE // 4 + 1) * 4
    first_cell = (jnp.arange(pairs)[:, None] == 0) & (jnp.arange(4)[None, :] == 0)
    sizes = jnp.where(first_cell, TILE, sizes)
    slot_number = jnp.array([0, 1, 0, 1], jnp.int32)[None, :]
    holder = jnp.where(jnp.array([True, True, False, False])[None, :], left[:, None], right[:, None])
    live = slot_number < holder
    return jnp.where(live, sizes, 0).reshape(IMAGE_SLOTS).astype(jnp.int32)


def shard_levels(rng, shape, shards, least, high):
    def one(position, parts):
        heights = jax.random.uniform(jax.random.fold_in(jax.random.fold_in(rng, 6), position), (parts,), jnp.float32, least / len(shards), high / len(shards))
        return jnp.repeat(jnp.exp(heights), shape[position] // parts).reshape((-1,) + (1,) * (len(shape) - position - 1))

    loudness = one(*shards[0])
    for cut in shards[1:]:
        loudness = loudness * one(*cut)
    return loudness


def gaussian(key, shape, deviation, bound, pieces=(), kind=jnp.bfloat16):
    values = jax.random.normal(key, shape, jnp.float32) * deviation
    if len(pieces) > 0:
        values = shard_levels(key, shape, pieces, -0.22, 0.18) * values
    return jnp.clip(values, min=-bound, max=bound).astype(kind)


def setup_inputs(seed: int = 0) -> dict:
    streams_of = jax.random.split(jax.random.key(seed), 13)
    return {
        "patches": draw_patches(jax.random.fold_in(streams_of[12], 71), 0),
        "counts": draw_counts(jax.random.fold_in(streams_of[12], 71), 0),
        "first_gain": jnp.clip(1.0 + 0.18 * jax.random.normal(streams_of[2], (D,), jnp.float32), 0.1, 1.9),
        "first_shift": gaussian(streams_of[3], (D,), 0.5, 3.0, (), jnp.float32),
        "in_weight": gaussian(streams_of[4], (D, 3, D), D ** -0.5, 0.15625, ((2, 4),)),
        "in_bias": draw_in_bias(jax.random.fold_in(streams_of[12], 71), 0),
        "out_weight": gaussian(streams_of[6], (D, D), D ** -0.5, 0.15625, ((1, 4),)),
        "out_bias": gaussian(streams_of[7], (D,), 0.5, 3.0, ((0, 4),), jnp.float32),
        "second_gain": jnp.clip(1.0 + 0.18 * jax.random.normal(streams_of[8], (D,), jnp.float32), 0.1, 1.9),
        "second_shift": gaussian(streams_of[9], (D,), 0.5, 3.0, ((0, 4),), jnp.float32),
        "merger_weight": gaussian(streams_of[10], (4, D, LLMW), (4 * D) ** -0.5, 0.078125, ((1, 4), (2, 8))),
        "merger_bias": gaussian(streams_of[11], (LLMW,), 1.0, 4.0, (), jnp.float32),
    }


EPS = 1e-06
MASKED = -1e+30

def layer_norm(values, gain, shift):
    row_mean = lax.optimization_barrier(jnp.mean(values, axis=-1, keepdims=True))
    centred = values - row_mean
    spread = lax.optimization_barrier(jnp.mean(centred * centred, axis=-1, keepdims=True))
    return centred * lax.rsqrt(spread + EPS) * gain + shift

def reference(patches, counts, first_gain, first_shift, in_weight, in_bias, out_weight, out_bias, second_gain, second_shift, merger_weight, merger_bias):
    head_size = D // HEADS
    scale = 1.0 / math.sqrt(head_size)
    block = D // N_TENSOR
    slot_view = patches.reshape(IMAGE_SLOTS, TILE, D)
    positions = jnp.arange(TILE, dtype=jnp.int32)
    merged_index = jnp.arange(TILE // 4, dtype=jnp.int32)

    def encode_slot(operand):
        tile, count = operand
        values = tile.astype(jnp.float32)
        normed = layer_norm(values, first_gain, first_shift).astype(jnp.bfloat16)
        projected = jnp.dot(normed, in_weight.reshape(D, 3 * D), preferred_element_type=jnp.float32) + in_bias.reshape(3 * D)
        projected = projected.astype(jnp.bfloat16).reshape(TILE, 3, HEADS, head_size).astype(jnp.float32)
        scores = jnp.einsum('qhd,khd->hqk', projected[:, 0], projected[:, 1]) * scale
        scores = jnp.where((positions < count)[None, None, :], scores, MASKED)
        highest = lax.optimization_barrier(jnp.max(scores, axis=-1, keepdims=True))
        raised = jnp.exp(scores - highest)
        weights = (raised / lax.optimization_barrier(jnp.sum(raised, axis=-1, keepdims=True))).astype(jnp.bfloat16)
        heads_out = jnp.einsum('hqk,khd->qhd', weights.astype(jnp.float32), projected[:, 2])
        heads_out = heads_out.astype(jnp.bfloat16).reshape(TILE, D)
        residual = values + jnp.dot(heads_out, out_weight, preferred_element_type=jnp.float32) + out_bias
        row_mean = lax.optimization_barrier(jnp.sum(residual, axis=1, keepdims=True)) / D
        second = lax.optimization_barrier(jnp.sum(residual * residual, axis=1, keepdims=True)) / D
        encoded = (residual - row_mean) * lax.rsqrt(second - row_mean * row_mean + EPS) * second_gain + second_shift
        merged = encoded.astype(jnp.bfloat16).reshape(TILE // 4, 4, D)
        total = jnp.zeros((TILE // 4, LLMW), jnp.float32)
        for feature_block in range(N_TENSOR):
            lower = feature_block * block
            piece = merged[:, :, lower:lower + block].reshape(TILE // 4, 4 * block)
            rows = merger_weight[:, lower:lower + block, :].reshape(4 * block, LLMW)
            partial_value = jnp.dot(piece, rows, preferred_element_type=jnp.float32).astype(jnp.bfloat16)
            total = total + lax.optimization_barrier(partial_value).astype(jnp.float32)
        embedded = total + merger_bias
        keep = (merged_index * 4 < count)[:, None]
        return jnp.where(keep, embedded, 0.0).astype(jnp.bfloat16)

    def empty_slot(operand):
        return jnp.zeros((TILE // 4, LLMW), jnp.bfloat16)

    def one_slot(operand):
        return lax.cond(operand[1] > 0, encode_slot, empty_slot, operand)
    result = lax.map(one_slot, (slot_view, counts))
    return result.reshape(ROWS, LLMW)
```

```python
import math

import jax
import jax.numpy as jnp
from jax import lax
from jax.sharding import PartitionSpec as P

D = 1280
HEADS = 16
TILE = 512
SLOTS = 2
MERGE = 4

EPS = 1e-06
MASKED = -1e30


def swap(x, dp_flip=0, tensor_flip=0):
    width = lax.axis_size("tensor")
    total = lax.axis_size("dp") * width
    flip = dp_flip * width + tensor_flip
    return lax.ppermute(x, ("dp", "tensor"), [(i, i ^ flip) for i in range(total)])


def layer_norm(values, gain, shift):
    row_mean = jnp.mean(values, axis=-1, keepdims=True)
    centred = values - row_mean
    spread = jnp.mean(centred * centred, axis=-1, keepdims=True)
    return centred * lax.rsqrt(spread + EPS) * gain + shift


def spread_over_tensor(x):
    b = swap(x, 0, 2)
    a = swap(x, 0, 1)
    c = swap(b, 0, 1)
    return [x, a, b, c]


def relative(x, me, axis=0):
    return jnp.stack(
        [lax.dynamic_index_in_dim(x, jnp.bitwise_xor(me, i), axis, keepdims=False) for i in range(x.shape[axis])],
        axis=axis,
    )


def select_swap(flag, a, b):
    return jnp.where(flag, b, a), jnp.where(flag, a, b)


def per_device(
    patches,
    counts,
    first_gain,
    first_shift,
    in_weight,
    in_bias,
    out_weight,
    out_bias,
    second_gain,
    second_shift,
    merger_weight,
    merger_bias,
):
    rank = lax.axis_index("dp")
    me = lax.axis_index("tensor")
    ranks = lax.axis_size("dp")
    groups = lax.axis_size("tensor")
    width = patches.shape[1]
    head_size = D // HEADS
    heads = width // head_size
    rows = TILE // MERGE
    block_width = merger_weight.shape[2]

    columns = [merger_weight]
    bit = 4
    while bit < ranks:
        columns = columns + [swap(c, bit) for c in columns]
        bit *= 2

    mine = lax.dynamic_slice_in_dim(counts, rank * SLOTS, SLOTS)
    theirs = lax.dynamic_slice_in_dim(counts, jnp.bitwise_xor(rank, 1) * SLOTS, SLOTS)
    own = mine[0] > 0
    count = jnp.where(own, mine[0], theirs[1])
    moved = swap(patches[TILE:], 1)
    shard = jnp.where(own, patches[:TILE], moved)

    blocks = spread_over_tensor(shard)
    gain = relative(first_gain.reshape(groups, width), me).reshape(D)
    shift = relative(first_shift.reshape(groups, width), me).reshape(D)
    weight = relative(in_weight.reshape(groups, width, 3 * width), me).reshape(D, 3 * width)
    values = jnp.concatenate(blocks, axis=1).astype(jnp.float32)
    normed = layer_norm(values, gain, shift).astype(jnp.bfloat16)
    projected = jnp.dot(normed, weight, preferred_element_type=jnp.float32)
    projected = (projected + in_bias.reshape(3 * width)).astype(jnp.bfloat16)
    projected = projected.reshape(TILE, 3, heads, head_size)
    scores = jnp.einsum(
        "qhd,khd->hqk", projected[:, 0], projected[:, 1], preferred_element_type=jnp.float32
    ) * (1.0 / math.sqrt(head_size))
    live = jnp.arange(TILE, dtype=jnp.int32) < count
    scores = jnp.where(live, scores, MASKED)
    highest = jnp.max(scores, axis=-1, keepdims=True)
    raised = jnp.exp(scores - highest)
    weights = (raised / jnp.sum(raised, axis=-1, keepdims=True)).astype(jnp.bfloat16)
    heads_out = jnp.einsum(
        "hqk,khd->qhd", weights, projected[:, 2], preferred_element_type=jnp.float32
    )
    heads_out = heads_out.astype(jnp.bfloat16).reshape(TILE, width)

    all_heads = jnp.concatenate(spread_over_tensor(heads_out), axis=1)
    out_rel = relative(out_weight.reshape(groups, width, width), me).reshape(D, width)
    residual = (
        shard.astype(jnp.float32)
        + jnp.dot(all_heads, out_rel, preferred_element_type=jnp.float32)
        + out_bias
    )
    stats = jnp.stack([jnp.sum(residual, axis=1), jnp.sum(residual * residual, axis=1)])
    stats = stats + swap(stats, 0, 1) + swap(stats, 0, 2) + swap(stats, 0, 3)
    row_mean = (stats[0] / D)[:, None]
    second = (stats[1] / D)[:, None]
    encoded = (residual - row_mean) * lax.rsqrt(
        second - row_mean * row_mean + EPS
    ) * second_gain + second_shift
    merged = encoded.astype(jnp.bfloat16).reshape(rows, MERGE * width)

    images = jnp.concatenate([merged] + [swap(merged, i) for i in (1, 2, 3)], axis=0)
    held = jnp.concatenate([c.reshape(MERGE * width, block_width) for c in columns], axis=1)
    total = held.shape[1]
    product = jnp.dot(images, held, preferred_element_type=jnp.float32).astype(jnp.bfloat16)

    low = jnp.bitwise_and(me, 1) == 1
    high = jnp.right_shift(me, 1) == 1
    product = product.reshape(4, 2, rows // 2, total)
    kept, sent = select_swap(low, product[:, 0], product[:, 1])
    half = kept.astype(jnp.float32) + swap(sent, 0, 1).astype(jnp.float32)
    half = half.reshape(2, 2, rows // 2, total)
    kept, sent = select_swap(high, half[:, 0], half[:, 1])
    bias = lax.dynamic_index_in_dim(
        merger_bias.reshape(ranks // 4, 4, block_width), jnp.bitwise_and(rank, 3), 1, keepdims=False
    )
    bias = relative(bias, jnp.right_shift(rank, 2)).reshape(total)
    summed = kept + swap(sent.astype(jnp.bfloat16), 0, 2).astype(jnp.float32) + bias
    summed = summed.astype(jnp.bfloat16)

    pieces = [summed[0], swap(summed[0], 1, 2), swap(summed[1], 2, 0), swap(summed[1], 3, 2)]
    pieces = jnp.stack(pieces).reshape(4, rows // 2, ranks // 4, block_width)
    for axis_bit in range(2):
        flag = jnp.bitwise_and(jnp.right_shift(rank, axis_bit), 1) == 1
        pair = pieces.reshape((2, 2) + pieces.shape[1:])
        pieces = jnp.where(flag, jnp.flip(pair, 1 - axis_bit), pair).reshape(pieces.shape)
    upper = ranks // 4
    place = 1
    while place < upper:
        flag = jnp.bitwise_and(jnp.right_shift(rank, 2), place) > 0
        split = pieces.reshape(4, rows // 2, upper // (2 * place), 2, place, block_width)
        pieces = jnp.where(flag, jnp.flip(split, 3), split).reshape(pieces.shape)
        place *= 2
    mixed = jnp.transpose(pieces, (1, 2, 0, 3)).reshape(rows // 2, merger_bias.shape[0])
    slot = jnp.right_shift(me, 1)
    within = jnp.bitwise_and(me, 1) * (rows // 2) + jnp.arange(rows // 2, dtype=jnp.int32)
    row_count = lax.dynamic_index_in_dim(mine, slot, 0, keepdims=False)
    keep = (within * MERGE < row_count)[:, None]
    return jnp.where(keep, mixed, jnp.zeros_like(mixed))


def solution(mesh):
    return jax.shard_map(
        per_device,
        mesh=mesh,
        in_specs=(
            P("dp", "tensor"),
            P(),
            P(),
            P(),
            P(None, None, "tensor"),
            P(None, "tensor"),
            P(None, "tensor"),
            P("tensor"),
            P("tensor"),
            P("tensor"),
            P(None, "tensor", "dp"),
            P(),
        ),
        out_specs=P(("dp", "tensor"), None),
        check_vma=False,
    )
```

```python
import functools
import math

import jax
import jax.numpy as jnp
from jax import lax
from jax.experimental import pallas as pl
from jax.experimental.pallas import tpu as pltpu
from jax.sharding import PartitionSpec as P

D = 1280
HEADS = 16
TILE = 512
SLOTS = 2
MERGE = 4

EPS = 1e-06
MASKED = -1e30


def swap(x, dp_flip=0, tensor_flip=0):
    width = lax.axis_size("tensor")
    total = lax.axis_size("dp") * width
    flip = dp_flip * width + tensor_flip
    return lax.ppermute(x, ("dp", "tensor"), [(i, i ^ flip) for i in range(total)])


def attend_kernel(scalars, own, near, far, cross, gain, shift, weight, bias, order, out, normed):
    me = scalars[0]
    count = scalars[1]
    rows, width = own.shape
    head_size = D // HEADS
    heads = width // head_size
    step = 32
    odd = jnp.bitwise_and(me, 1) == 1
    upper = jnp.bitwise_and(me, 2) == 2
    for start in range(0, rows, step):
        part = pl.ds(start, step)
        blocks = [r[part, :].astype(jnp.float32) for r in (own, near, far, cross)]
        mean = sum(jnp.sum(b, axis=1, keepdims=True) for b in blocks) / D
        centred = [b - mean for b in blocks]
        spread = sum(jnp.sum(c * c, axis=1, keepdims=True) for c in centred) / D
        inverse = lax.rsqrt(spread + EPS)
        p, q, r, s = [c * inverse for c in centred]
        p, q, r, s = jnp.where(odd, q, p), jnp.where(odd, p, q), jnp.where(odd, s, r), jnp.where(odd, r, s)
        p, q, r, s = jnp.where(upper, r, p), jnp.where(upper, s, q), jnp.where(upper, p, r), jnp.where(upper, q, s)
        line = jnp.concatenate([p, q, r, s], axis=1)
        normed[part, :] = (line * gain[...] + shift[...]).astype(jnp.bfloat16)
    projected = lax.dot_general(
        weight[...], normed[...], (((1,), (1,)), ((), ())), preferred_element_type=jnp.float32
    )
    projected = (projected + bias[...]).astype(jnp.bfloat16)
    queries = jnp.dot(
        projected[:width], order[...], preferred_element_type=jnp.float32
    ).astype(jnp.bfloat16)
    live = lax.broadcasted_iota(jnp.int32, (rows, rows), 0) < count
    scale = math.log2(math.e) / math.sqrt(head_size)
    for h in range(heads):
        a, b = h * head_size, (h + 1) * head_size
        scores = lax.dot_general(
            projected[width + a : width + b], queries[a:b], (((0,), (0,)), ((), ())),
            preferred_element_type=jnp.float32,
        )
        scores = jnp.where(live, scores, MASKED)
        highest = jnp.max(scores, axis=0, keepdims=True)
        raised = jnp.exp2((scores - highest) * scale)
        total = jnp.sum(raised, axis=0, keepdims=True)
        mixed = jnp.dot(
            projected[2 * width + a : 2 * width + b], raised.astype(jnp.bfloat16),
            preferred_element_type=jnp.float32,
        )
        out[a:b, :] = (mixed / total).astype(jnp.bfloat16)


def attend(scalars, blocks, gain, shift, weight, bias, order):
    rows, width = blocks[0].shape
    vm = pl.BlockSpec(memory_space=pltpu.VMEM)
    return pl.pallas_call(
        attend_kernel,
        out_shape=jax.ShapeDtypeStruct((width, rows), jnp.bfloat16),
        in_specs=[pl.BlockSpec(memory_space=pltpu.SMEM)] + [vm] * 9,
        out_specs=vm,
        scratch_shapes=[pltpu.VMEM((rows, D), jnp.bfloat16)],
    )(scalars, *blocks, gain, shift, weight, bias, order)


def spread_over_tensor(x):
    b = swap(x, 0, 2)
    a = swap(x, 0, 1)
    c = swap(b, 0, 1)
    return [x, a, b, c]


def relative(x, me, axis=0):
    return jnp.stack(
        [lax.dynamic_index_in_dim(x, jnp.bitwise_xor(me, i), axis, keepdims=False) for i in range(x.shape[axis])],
        axis=axis,
    )


def select_swap(flag, a, b):
    return jnp.where(flag, b, a), jnp.where(flag, a, b)


def place_kernel(block_width, scalars, p0, p1, p2, p3, out):
    rank = scalars[0]
    rows, total = p0.shape
    keep = lax.broadcasted_iota(jnp.int32, (rows, block_width), 0) < scalars[1]
    for m in range(total // block_width):
        upper = jnp.bitwise_xor(jnp.right_shift(rank, 2), m) * 4
        for d, piece in enumerate((p0, p1, p2, p3)):
            column = upper + jnp.bitwise_xor(jnp.bitwise_and(rank, 3), d)
            block = piece[:, m * block_width : (m + 1) * block_width]
            block = jnp.where(keep, block, jnp.zeros_like(block))
            start = pl.multiple_of(column * block_width, block_width)
            out[:, pl.ds(start, block_width)] = block


def place(scalars, pieces, block_width):
    rows, total = pieces[0].shape
    rank, live_rows = scalars
    if block_width % 128 == 0:
        vmem = pl.BlockSpec(memory_space=pltpu.VMEM)
        return pl.pallas_call(
            functools.partial(place_kernel, block_width),
            out_shape=jax.ShapeDtypeStruct((rows, 4 * total), pieces[0].dtype),
            in_specs=[pl.BlockSpec(memory_space=pltpu.SMEM)] + [vmem] * 4,
            out_specs=vmem,
        )(jnp.stack(scalars), *pieces)
    upper = total // block_width
    pieces = jnp.stack(pieces).reshape(4, rows, upper, block_width)
    pieces = relative(pieces, jnp.bitwise_and(rank, 3), 0)
    pieces = relative(pieces, jnp.right_shift(rank, 2), 2)
    mixed = jnp.transpose(pieces, (1, 2, 0, 3)).reshape(rows, 4 * total)
    keep = jnp.arange(rows, dtype=jnp.int32)[:, None] < live_rows
    return jnp.where(keep, mixed, jnp.zeros_like(mixed))


def compute(
    patches,
    counts,
    first_gain,
    first_shift,
    in_weight,
    in_bias,
    out_weight,
    out_bias,
    second_gain,
    second_shift,
    merger_weight,
    merger_bias,
):
    rank = lax.axis_index("dp")
    me = lax.axis_index("tensor")
    ranks = lax.axis_size("dp")
    groups = lax.axis_size("tensor")
    width = patches.shape[1]
    rows = TILE // MERGE
    block_width = merger_weight.shape[2]

    columns = [merger_weight]
    bit = 4
    while bit < ranks:
        columns = columns + [swap(c, bit) for c in columns]
        bit *= 2

    mine = lax.dynamic_slice_in_dim(counts, rank * SLOTS, SLOTS)
    theirs = lax.dynamic_slice_in_dim(counts, jnp.bitwise_xor(rank, 1) * SLOTS, SLOTS)
    own = mine[0] > 0
    count = jnp.where(own, mine[0], theirs[1])
    moved = swap(patches[TILE:], 1)
    shard = jnp.where(own, patches[:TILE], moved)

    source = jnp.arange(TILE, dtype=jnp.int32)
    order = (source % MERGE * rows + source // MERGE)[:, None] == source[None, :]
    heads_out = attend(
        jnp.stack([me, count]),
        spread_over_tensor(shard),
        first_gain[None],
        first_shift[None],
        jnp.transpose(in_weight, (1, 2, 0)).reshape(3 * width, D),
        in_bias.reshape(3 * width, 1),
        order.astype(jnp.bfloat16),
    )
    base = jnp.transpose(shard.reshape(rows, MERGE, width), (1, 0, 2)).reshape(TILE, width)
    base = base.astype(jnp.float32) + out_bias

    all_heads = jnp.concatenate(spread_over_tensor(heads_out), axis=0)
    out_rel = relative(out_weight.reshape(groups, width, width), me).reshape(D, width)
    residual = base + lax.dot_general(
        all_heads, out_rel, (((0,), (0,)), ((), ())), preferred_element_type=jnp.float32
    )
    stats = jnp.stack([jnp.sum(residual, axis=1), jnp.sum(residual * residual, axis=1)])
    stats = stats + swap(stats, 0, 1) + swap(stats, 0, 2) + swap(stats, 0, 3)
    row_mean = (stats[0] / D)[:, None]
    second = (stats[1] / D)[:, None]
    encoded = (residual - row_mean) * lax.rsqrt(
        second - row_mean * row_mean + EPS
    ) * second_gain + second_shift
    merged = encoded.astype(jnp.bfloat16).reshape(MERGE, rows, width)
    merged = jnp.transpose(merged, (1, 0, 2)).reshape(rows, MERGE * width)

    images = jnp.concatenate([merged] + [swap(merged, i) for i in (1, 2, 3)], axis=0)
    held = jnp.concatenate([c.reshape(MERGE * width, block_width) for c in columns], axis=1)
    total = held.shape[1]
    product = jnp.dot(images, held, preferred_element_type=jnp.float32).astype(jnp.bfloat16)

    low = jnp.bitwise_and(me, 1) == 1
    high = jnp.right_shift(me, 1) == 1
    product = product.reshape(4, 2, rows // 2, total)
    kept, sent = select_swap(low, product[:, 0], product[:, 1])
    half = kept.astype(jnp.float32) + swap(sent, 0, 1).astype(jnp.float32)
    half = half.reshape(2, 2, rows // 2, total)
    kept, sent = select_swap(high, half[:, 0], half[:, 1])
    bias = lax.dynamic_index_in_dim(
        merger_bias.reshape(ranks // 4, 4, block_width), jnp.bitwise_and(rank, 3), 1, keepdims=False
    )
    bias = relative(bias, jnp.right_shift(rank, 2)).reshape(total)
    summed = kept + swap(sent.astype(jnp.bfloat16), 0, 2).astype(jnp.float32) + bias
    summed = summed.astype(jnp.bfloat16)

    pieces = [summed[0], swap(summed[0], 1, 2), swap(summed[1], 2, 0), swap(summed[1], 3, 2)]
    slot = jnp.right_shift(me, 1)
    row_count = lax.dynamic_index_in_dim(mine, slot, 0, keepdims=False)
    first_row = jnp.bitwise_and(me, 1) * (rows // 2)
    live_rows = jnp.right_shift(row_count, 2) - first_row
    return place((rank, live_rows), pieces, block_width)


def solution(mesh):
    return jax.shard_map(
        compute,
        mesh=mesh,
        in_specs=(
            P("dp", "tensor"),
            P(),
            P(),
            P(),
            P(None, None, "tensor"),
            P(None, "tensor"),
            P(None, "tensor"),
            P("tensor"),
            P("tensor"),
            P("tensor"),
            P(None, "tensor", "dp"),
            P(),
        ),
        out_specs=P(("dp", "tensor"), None),
        check_vma=False,
    )
```

```python
import functools
import math

import jax
import jax.numpy as jnp
from jax import lax
from jax.experimental import pallas as pl
from jax.experimental.pallas import tpu as pltpu
from jax.sharding import PartitionSpec as P

D = 1280
HEADS = 16
TILE = 512
SLOTS = 2
MERGE = 4
LANES = 128

EPS = 1e-06
MASKED = -1e30


VMEM = pl.BlockSpec(memory_space=pltpu.VMEM)
SMEM = pl.BlockSpec(memory_space=pltpu.SMEM)


def swap(x, dp_flip=0, tensor_flip=0):
    width = lax.axis_size("tensor")
    total = lax.axis_size("dp") * width
    flip = dp_flip * width + tensor_flip
    return lax.ppermute(x, ("dp", "tensor"), [(i, i ^ flip) for i in range(total)])


def spread_over_tensor(x):
    far = swap(x, 0, 2)
    return [x, swap(x, 0, 1), far, swap(far, 0, 1)]


def relative(x, me, axis=0):
    return jnp.stack(
        [
            lax.dynamic_index_in_dim(x, jnp.bitwise_xor(me, i), axis, keepdims=False)
            for i in range(x.shape[axis])
        ],
        axis=axis,
    )


def reorder(me, blocks):
    p, q, r, s = blocks
    odd = jnp.bitwise_and(me, 1) == 1
    upper = jnp.bitwise_and(me, 2) == 2
    p, q, r, s = jnp.where(odd, q, p), jnp.where(odd, p, q), jnp.where(odd, s, r), jnp.where(odd, r, s)
    return [
        jnp.where(upper, r, p),
        jnp.where(upper, s, q),
        jnp.where(upper, p, r),
        jnp.where(upper, q, s),
    ]


def near_core(x):
    return pltpu.with_memory_space_constraint(x, pltpu.VMEM)


def attend_kernel(scalars, own, near, far, cross, vectors, weight, order, out, normed, projected, columns):
    me = scalars[0]
    count = scalars[1]
    width, rows = own.shape
    size = D // HEADS
    blocks = (own, near, far, cross)
    columns[...] = jnp.transpose(vectors[...])
    step = 32
    total = jnp.zeros((8, rows), jnp.float32)
    for r in blocks:
        for start in range(0, width, step):
            x = r[start : start + step, :].astype(jnp.float32)
            for i in range(0, step, 8):
                total += x[i : i + 8]
    mean = jnp.sum(total, axis=0, keepdims=True) / D
    total = jnp.zeros((8, rows), jnp.float32)
    for r in blocks:
        for start in range(0, width, step):
            x = r[start : start + step, :].astype(jnp.float32) - mean
            x = x * x
            for i in range(0, step, 8):
                total += x[i : i + 8]
    inverse = lax.rsqrt(jnp.sum(total, axis=0, keepdims=True) / D + EPS)
    for i, r in enumerate(blocks):
        first = jnp.bitwise_xor(me, i) * width
        for start in range(0, width, step):
            part = pl.ds(pl.multiple_of(first + start, step), step)
            line = (r[start : start + step, :].astype(jnp.float32) - mean) * inverse
            normed[part, :] = (line * columns[part, 0:1] + columns[part, 1:2]).astype(jnp.bfloat16)
    scale = math.log2(math.e) / math.sqrt(size)
    for p in range(3):
        part = slice(p * width, (p + 1) * width)
        got = jnp.dot(weight[part, :], normed[...], preferred_element_type=jnp.float32) + columns[part, 2:3]
        projected[part, :] = (got * scale if p == 0 else got).astype(jnp.bfloat16)
    queries = jnp.dot(projected[:width, :], order[...], preferred_element_type=jnp.float32)
    projected[:width, :] = queries.astype(jnp.bfloat16)
    place = lax.broadcasted_iota(jnp.int32, (16, rows), 1)
    first = lax.broadcasted_iota(jnp.int32, (16, rows), 0) == 0
    dead = jnp.where((place >= count) & first, MASKED, 0.0).astype(jnp.bfloat16)
    ones = jnp.ones((16, rows), jnp.bfloat16)
    for h in range(width // size):
        part = slice(h * size, (h + 1) * size)
        queries = jnp.concatenate([projected[part, :], ones], axis=0)
        keys = projected[width + h * size : width + (h + 1) * size, :]
        keys = jnp.concatenate([keys, dead], axis=0)
        values = projected[2 * width + h * size : 2 * width + (h + 1) * size, :]
        for c in range(0, rows, 256):
            scores = lax.dot_general(
                keys, queries[:, c : c + 256], (((0,), (0,)), ((), ())), preferred_element_type=jnp.float32
            )
            raised = jnp.exp2(scores - jnp.max(scores, axis=0, keepdims=True))
            total = jnp.sum(raised, axis=0, keepdims=True)
            mixed = jnp.dot(values, raised.astype(jnp.bfloat16), preferred_element_type=jnp.float32)
            out[part, c : c + 256] = (mixed / total).astype(jnp.bfloat16)


def attend(scalars, blocks, vectors, weight, order):
    width, rows = blocks[0].shape
    operands = [near_core(x) for x in (*blocks, vectors, staged(weight), order)]
    return pl.pallas_call(
        attend_kernel,
        out_shape=pltpu.VMEM((width, rows), jnp.bfloat16),
        in_specs=[SMEM] + [VMEM] * 7,
        out_specs=VMEM,
        scratch_shapes=[
            pltpu.VMEM((D, rows), jnp.bfloat16),
            pltpu.VMEM((3 * width, rows), jnp.bfloat16),
            pltpu.VMEM((D, vectors.shape[0]), jnp.float32),
        ],
        compiler_params=pltpu.CompilerParams(vmem_limit_bytes=20 << 20),
    )(scalars, *operands)


def stage_kernel(source, out):
    pltpu.sync_copy(source, out)


def staged(x):
    return pl.pallas_call(
        stage_kernel,
        out_shape=pltpu.VMEM(x.shape, x.dtype),
        in_specs=[pl.BlockSpec(memory_space=pl.ANY)],
        out_specs=VMEM,
        compiler_params=pltpu.CompilerParams(vmem_limit_bytes=8 << 20),
    )(x)


def place_kernel(block_width, scalars, p0, p1, p2, p3, out):
    rank = scalars[0]
    rows, total = p0.shape
    keep = lax.broadcasted_iota(jnp.int32, (rows, block_width), 0) < scalars[1]
    for m in range(total // block_width):
        upper = jnp.bitwise_xor(jnp.right_shift(rank, 2), m) * 4
        for d, piece in enumerate((p0, p1, p2, p3)):
            column = upper + jnp.bitwise_xor(jnp.bitwise_and(rank, 3), d)
            block = piece[:, m * block_width : (m + 1) * block_width]
            block = jnp.where(keep, block, jnp.zeros_like(block))
            start = pl.multiple_of(column * block_width, block_width)
            out[:, pl.ds(start, block_width)] = block


def place(scalars, pieces, block_width):
    rows, total = pieces[0].shape
    rank, live_rows = scalars
    if block_width % LANES == 0:
        return pl.pallas_call(
            functools.partial(place_kernel, block_width),
            out_shape=jax.ShapeDtypeStruct((rows, 4 * total), pieces[0].dtype),
            in_specs=[SMEM] + [VMEM] * 4,
            out_specs=VMEM,
            compiler_params=pltpu.CompilerParams(vmem_limit_bytes=12 << 20),
        )(jnp.stack(scalars), *[near_core(x) for x in pieces])
    upper = total // block_width
    pieces = jnp.stack(pieces).reshape(4, rows, upper, block_width)
    pieces = relative(pieces, jnp.bitwise_and(rank, 3), 0)
    pieces = relative(pieces, jnp.right_shift(rank, 2), 2)
    mixed = jnp.transpose(pieces, (1, 2, 0, 3)).reshape(rows, 4 * total)
    keep = jnp.arange(rows, dtype=jnp.int32)[:, None] < live_rows
    return jnp.where(keep, mixed, jnp.zeros_like(mixed))


def compute(
    patches,
    counts,
    first_gain,
    first_shift,
    in_weight,
    in_bias,
    out_weight,
    out_bias,
    second_gain,
    second_shift,
    merger_weight,
    merger_bias,
):
    rank = lax.axis_index("dp")
    me = lax.axis_index("tensor")
    ranks = lax.axis_size("dp")
    width = patches.shape[1]
    rows = TILE // MERGE
    block_width = merger_weight.shape[2]

    features = jnp.transpose(patches)

    mine = lax.dynamic_slice_in_dim(counts, rank * SLOTS, SLOTS)
    theirs = lax.dynamic_slice_in_dim(counts, jnp.bitwise_xor(rank, 1) * SLOTS, SLOTS)
    own = mine[0] > 0
    count = jnp.where(own, mine[0], theirs[1])
    moved = swap(features[:, TILE:], 1)
    shard = jnp.where(own, lax.optimization_barrier(features[:, :TILE]), moved)
    scalars = jnp.stack([me, count])

    columns = [merger_weight]
    bit = 4
    while bit < ranks:
        columns = columns + [swap(c, bit) for c in columns]
        bit *= 2
    held = jnp.concatenate([c.reshape(MERGE * width, block_width) for c in columns], axis=1)

    source = jnp.arange(TILE, dtype=jnp.int32)
    order = (source % MERGE * rows + source // MERGE)[:, None] == source[None, :]
    order = order.astype(jnp.bfloat16)
    vectors = [first_gain, first_shift, jnp.pad(in_bias.reshape(3 * width), (0, D - 3 * width))]
    vectors = jnp.pad(jnp.stack(vectors), ((0, 5), (0, 0)))
    heads_out = attend(
        scalars,
        spread_over_tensor(shard),
        vectors,
        jnp.transpose(in_weight, (1, 2, 0)).reshape(3 * width, D),
        order,
    )
    base = jnp.dot(shard, order, preferred_element_type=jnp.float32) + out_bias[:, None]
    all_heads = jnp.concatenate(reorder(me, spread_over_tensor(heads_out)), axis=0)
    residual = base + jnp.dot(
        jnp.transpose(out_weight), all_heads, preferred_element_type=jnp.float32
    )
    stats = jnp.stack([jnp.sum(residual, axis=0), jnp.sum(residual * residual, axis=0)])
    stats = stats + swap(stats, 0, 1) + swap(stats, 0, 2) + swap(stats, 0, 3)
    row_mean = stats[0] / D
    second = stats[1] / D
    encoded = (residual - row_mean) * lax.rsqrt(
        second - row_mean * row_mean + EPS
    ) * second_gain[:, None] + second_shift[:, None]
    merged = encoded.astype(jnp.bfloat16).reshape(width, MERGE, rows)
    merged = jnp.transpose(merged, (1, 0, 2)).reshape(MERGE * width, rows)

    one = swap(merged, 1)
    two = swap(merged, 2)
    cut = MERGE * width // 2
    three = swap(two[:cut], 1)
    three = jnp.concatenate([three, swap(one[cut:], 2)], axis=0)

    high = jnp.right_shift(me, 1) == 1
    bias = lax.dynamic_index_in_dim(
        merger_bias.reshape(ranks // 4, 4, block_width), jnp.bitwise_and(rank, 3), 1, keepdims=False
    )
    bias = relative(bias, jnp.right_shift(rank, 2)).reshape(ranks // 4 * block_width)

    low = jnp.bitwise_and(me, 1) == 1

    def reduced(first, second, before=None):
        lines = jnp.concatenate([first, second], axis=1)
        product = lax.dot_general(
            lines, held, (((0,), (0,)), ((), ())), preferred_element_type=jnp.float32
        ).reshape(2, 2, rows // 2, held.shape[1])
        sent = jnp.where(low, product[:, 0], product[:, 1]).astype(jnp.bfloat16)
        kept = jnp.where(low, product[:, 1], product[:, 0])
        half = kept + swap(sent, 0, 1).astype(jnp.float32)
        kept = jnp.where(high, half[1], half[0])
        sent = jnp.where(high, half[0], half[1]).astype(jnp.bfloat16)
        if before is not None:
            sent, before = lax.optimization_barrier((sent, before))
        other = swap(sent, 0, 2)
        total = kept + other.astype(jnp.float32)
        return (total + bias).astype(jnp.bfloat16), before

    near, _ = reduced(merged, one)
    pair, near = reduced(two, three, near)
    pieces = [near, swap(near, 1, 2)]
    pieces += [swap(pair, 2, 0), swap(pair, 3, 2)]

    slot = jnp.right_shift(me, 1)
    row_count = lax.dynamic_index_in_dim(mine, slot, 0, keepdims=False)
    first_row = jnp.bitwise_and(me, 1) * (rows // 2)
    live_rows = jnp.right_shift(row_count, 2) - first_row
    return place((rank, live_rows), pieces, block_width)


def solution(mesh):
    return jax.shard_map(
        compute,
        mesh=mesh,
        in_specs=(
            P("dp", "tensor"),
            P(),
            P(),
            P(),
            P(None, None, "tensor"),
            P(None, "tensor"),
            P(None, "tensor"),
            P("tensor"),
            P("tensor"),
            P("tensor"),
            P(None, "tensor", "dp"),
            P(),
        ),
        out_specs=P(("dp", "tensor"), None),
        check_vma=False,
    )
```

```python
import functools
import math

import jax
import jax.numpy as jnp
from jax import lax
from jax.experimental import pallas as pl
from jax.experimental.pallas import tpu as pltpu
from jax.sharding import PartitionSpec as P

D = 1280
HEADS = 16
TILE = 512
SLOTS = 2
MERGE = 4
LANES = 128

EPS = 1e-06
MASKED = -1e30


VMEM = pl.BlockSpec(memory_space=pltpu.VMEM)
SMEM = pl.BlockSpec(memory_space=pltpu.SMEM)


def swap(x, dp_flip=0, tensor_flip=0):
    width = lax.axis_size("tensor")
    total = lax.axis_size("dp") * width
    flip = dp_flip * width + tensor_flip
    return lax.ppermute(x, ("dp", "tensor"), [(i, i ^ flip) for i in range(total)])


def spread_over_tensor(x):
    far = swap(x, 0, 2)
    return [x, swap(x, 0, 1), far, swap(far, 0, 1)]


def relative(x, me, axis=0):
    return jnp.stack(
        [
            lax.dynamic_index_in_dim(x, jnp.bitwise_xor(me, i), axis, keepdims=False)
            for i in range(x.shape[axis])
        ],
        axis=axis,
    )


def reorder(me, blocks):
    p, q, r, s = blocks
    odd = jnp.bitwise_and(me, 1) == 1
    upper = jnp.bitwise_and(me, 2) == 2
    p, q, r, s = jnp.where(odd, q, p), jnp.where(odd, p, q), jnp.where(odd, s, r), jnp.where(odd, r, s)
    return [
        jnp.where(upper, r, p),
        jnp.where(upper, s, q),
        jnp.where(upper, p, r),
        jnp.where(upper, q, s),
    ]


def near_core(x):
    return pltpu.with_memory_space_constraint(x, pltpu.VMEM)


def attend_kernel(scalars, own, near, far, cross, vectors, weight, order, out, normed, projected, columns):
    me = scalars[0]
    count = scalars[1]
    width, rows = own.shape
    size = D // HEADS
    blocks = (own, near, far, cross)
    columns[...] = jnp.transpose(vectors[...])
    step = 32
    total = jnp.zeros((8, rows), jnp.float32)
    for r in blocks:
        for start in range(0, width, step):
            x = r[start : start + step, :].astype(jnp.float32)
            for i in range(0, step, 8):
                total += x[i : i + 8]
    mean = jnp.sum(total, axis=0, keepdims=True) / D
    total = jnp.zeros((8, rows), jnp.float32)
    for r in blocks:
        for start in range(0, width, step):
            x = r[start : start + step, :].astype(jnp.float32) - mean
            x = x * x
            for i in range(0, step, 8):
                total += x[i : i + 8]
    inverse = lax.rsqrt(jnp.sum(total, axis=0, keepdims=True) / D + EPS)
    for i, r in enumerate(blocks):
        first = jnp.bitwise_xor(me, i) * width
        for start in range(0, width, step):
            part = pl.ds(pl.multiple_of(first + start, step), step)
            line = (r[start : start + step, :].astype(jnp.float32) - mean) * inverse
            normed[part, :] = (line * columns[part, 0:1] + columns[part, 1:2]).astype(jnp.bfloat16)
    scale = math.log2(math.e) / math.sqrt(size)
    for p in range(3):
        part = slice(p * width, (p + 1) * width)
        got = jnp.dot(weight[part, :], normed[...], preferred_element_type=jnp.float32) + columns[part, 2:3]
        projected[part, :] = (got * scale if p == 0 else got).astype(jnp.bfloat16)
    queries = jnp.dot(projected[:width, :], order[...], preferred_element_type=jnp.float32)
    projected[:width, :] = queries.astype(jnp.bfloat16)
    place = lax.broadcasted_iota(jnp.int32, (16, rows), 1)
    first = lax.broadcasted_iota(jnp.int32, (16, rows), 0) == 0
    dead = jnp.where((place >= count) & first, MASKED, 0.0).astype(jnp.bfloat16)
    ones = jnp.ones((16, rows), jnp.bfloat16)
    for h in range(width // size):
        part = slice(h * size, (h + 1) * size)
        queries = jnp.concatenate([projected[part, :], ones], axis=0)
        keys = projected[width + h * size : width + (h + 1) * size, :]
        keys = jnp.concatenate([keys, dead], axis=0)
        values = projected[2 * width + h * size : 2 * width + (h + 1) * size, :]
        for c in range(0, rows, 256):
            scores = lax.dot_general(
                keys, queries[:, c : c + 256], (((0,), (0,)), ((), ())), preferred_element_type=jnp.float32
            )
            raised = jnp.exp2(scores - jnp.max(scores, axis=0, keepdims=True))
            total = jnp.sum(raised, axis=0, keepdims=True)
            mixed = jnp.dot(values, raised.astype(jnp.bfloat16), preferred_element_type=jnp.float32)
            out[part, c : c + 256] = (mixed / total).astype(jnp.bfloat16)


def attend(scalars, blocks, vectors, weight, order):
    width, rows = blocks[0].shape
    operands = [near_core(x) for x in (*blocks, vectors, staged(weight), order)]
    return pl.pallas_call(
        attend_kernel,
        out_shape=pltpu.VMEM((width, rows), jnp.bfloat16),
        in_specs=[SMEM] + [VMEM] * 7,
        out_specs=VMEM,
        scratch_shapes=[
            pltpu.VMEM((D, rows), jnp.bfloat16),
            pltpu.VMEM((3 * width, rows), jnp.bfloat16),
            pltpu.VMEM((D, vectors.shape[0]), jnp.float32),
        ],
        compiler_params=pltpu.CompilerParams(vmem_limit_bytes=20 << 20),
    )(scalars, *operands)


def stage_kernel(source, out):
    pltpu.sync_copy(source, out)


def staged(x):
    return pl.pallas_call(
        stage_kernel,
        out_shape=pltpu.VMEM(x.shape, x.dtype),
        in_specs=[pl.BlockSpec(memory_space=pl.ANY)],
        out_specs=VMEM,
        compiler_params=pltpu.CompilerParams(vmem_limit_bytes=8 << 20),
    )(x)


def join_kernel(*refs):
    sources, out, sems = refs[:-2], refs[-2], refs[-1]
    width = out.shape[1] // len(sources)
    copies = [
        pltpu.make_async_copy(source, out.at[:, i * width : (i + 1) * width], sems.at[i])
        for i, source in enumerate(sources)
    ]
    for copy in copies:
        copy.start()
    for copy in copies:
        copy.wait()


def joined(columns):
    rows, width = columns[0].shape
    if width % LANES > 0:
        return jnp.concatenate(columns, axis=1)
    return pl.pallas_call(
        join_kernel,
        out_shape=pltpu.VMEM((rows, width * len(columns)), columns[0].dtype),
        in_specs=[pl.BlockSpec(memory_space=pl.ANY)] * len(columns),
        out_specs=VMEM,
        scratch_shapes=[pltpu.SemaphoreType.DMA((len(columns),))],
        compiler_params=pltpu.CompilerParams(vmem_limit_bytes=8 << 20),
    )(*columns)


def place_kernel(block_width, scalars, p0, p1, p2, p3, out):
    rank = scalars[0]
    rows, total = p0.shape
    keep = lax.broadcasted_iota(jnp.int32, (rows, block_width), 0) < scalars[1]
    for m in range(total // block_width):
        upper = jnp.bitwise_xor(jnp.right_shift(rank, 2), m) * 4
        for d, piece in enumerate((p0, p1, p2, p3)):
            column = upper + jnp.bitwise_xor(jnp.bitwise_and(rank, 3), d)
            block = piece[:, m * block_width : (m + 1) * block_width]
            block = jnp.where(keep, block, jnp.zeros_like(block))
            start = pl.multiple_of(column * block_width, block_width)
            out[:, pl.ds(start, block_width)] = block


def place(scalars, pieces, block_width):
    rows, total = pieces[0].shape
    rank, live_rows = scalars
    if block_width % LANES == 0:
        return pl.pallas_call(
            functools.partial(place_kernel, block_width),
            out_shape=jax.ShapeDtypeStruct((rows, 4 * total), pieces[0].dtype),
            in_specs=[SMEM] + [VMEM] * 4,
            out_specs=VMEM,
            compiler_params=pltpu.CompilerParams(vmem_limit_bytes=12 << 20),
        )(jnp.stack(scalars), *[near_core(x) for x in pieces])
    upper = total // block_width
    pieces = jnp.stack(pieces).reshape(4, rows, upper, block_width)
    pieces = relative(pieces, jnp.bitwise_and(rank, 3), 0)
    pieces = relative(pieces, jnp.right_shift(rank, 2), 2)
    mixed = jnp.transpose(pieces, (1, 2, 0, 3)).reshape(rows, 4 * total)
    keep = jnp.arange(rows, dtype=jnp.int32)[:, None] < live_rows
    return jnp.where(keep, mixed, jnp.zeros_like(mixed))


def compute(
    patches,
    counts,
    first_gain,
    first_shift,
    in_weight,
    in_bias,
    out_weight,
    out_bias,
    second_gain,
    second_shift,
    merger_weight,
    merger_bias,
):
    rank = lax.axis_index("dp")
    me = lax.axis_index("tensor")
    ranks = lax.axis_size("dp")
    width = patches.shape[1]
    rows = TILE // MERGE
    block_width = merger_weight.shape[2]

    features = jnp.transpose(patches)

    mine = lax.dynamic_slice_in_dim(counts, rank * SLOTS, SLOTS)
    theirs = lax.dynamic_slice_in_dim(counts, jnp.bitwise_xor(rank, 1) * SLOTS, SLOTS)
    own = mine[0] > 0
    count = jnp.where(own, mine[0], theirs[1])
    moved = swap(features[:, TILE:], 1)
    shard = jnp.where(own, lax.optimization_barrier(features[:, :TILE]), moved)
    scalars = jnp.stack([me, count])

    columns = [merger_weight]
    bit = 4
    while bit < ranks:
        columns = columns + [swap(c, bit) for c in columns]
        bit *= 2
    held = joined([c.reshape(MERGE * width, block_width) for c in columns])

    source = jnp.arange(TILE, dtype=jnp.int32)
    order = (source % MERGE * rows + source // MERGE)[:, None] == source[None, :]
    order = order.astype(jnp.bfloat16)
    vectors = [first_gain, first_shift, jnp.pad(in_bias.reshape(3 * width), (0, D - 3 * width))]
    vectors = jnp.pad(jnp.stack(vectors), ((0, 5), (0, 0)))
    heads_out = attend(
        scalars,
        spread_over_tensor(shard),
        vectors,
        jnp.transpose(in_weight, (1, 2, 0)).reshape(3 * width, D),
        order,
    )
    base = jnp.dot(shard, order, preferred_element_type=jnp.float32) + out_bias[:, None]
    all_heads = jnp.concatenate(reorder(me, spread_over_tensor(heads_out)), axis=0)
    residual = base + jnp.dot(
        jnp.transpose(out_weight), all_heads, preferred_element_type=jnp.float32
    )
    stats = jnp.stack([jnp.sum(residual, axis=0), jnp.sum(residual * residual, axis=0)])
    stats = stats + swap(stats, 0, 1) + swap(stats, 0, 2) + swap(stats, 0, 3)
    row_mean = stats[0] / D
    second = stats[1] / D
    encoded = (residual - row_mean) * lax.rsqrt(
        second - row_mean * row_mean + EPS
    ) * second_gain[:, None] + second_shift[:, None]
    merged = encoded.astype(jnp.bfloat16).reshape(width, MERGE, rows)
    merged = jnp.transpose(merged, (1, 0, 2)).reshape(MERGE * width, rows)

    one = swap(merged, 1)
    two = swap(merged, 2)
    cut = MERGE * width * 3 // 8
    three = swap(two[:cut], 1)
    three = jnp.concatenate([three, swap(one[cut:], 2)], axis=0)

    high = jnp.right_shift(me, 1) == 1
    bias = lax.dynamic_index_in_dim(
        merger_bias.reshape(ranks // 4, 4, block_width), jnp.bitwise_and(rank, 3), 1, keepdims=False
    )
    bias = relative(bias, jnp.right_shift(rank, 2)).reshape(ranks // 4 * block_width)

    low = jnp.bitwise_and(me, 1) == 1

    def core_sum(lines):
        product = lax.dot_general(
            lines, held, (((0,), (0,)), ((), ())), preferred_element_type=jnp.float32
        ).reshape(-1, 2, rows // 2, held.shape[1])
        sent = jnp.where(low, product[:, 0], product[:, 1]).astype(jnp.bfloat16)
        kept = jnp.where(low, product[:, 1], product[:, 0])
        return kept + swap(sent, 0, 1).astype(jnp.float32)

    def reduced(first, second, before=None):
        kept = jnp.where(high, second, first)
        sent = jnp.where(high, first, second).astype(jnp.bfloat16)
        if before is not None:
            sent, before = lax.optimization_barrier((sent, before))
        other = swap(sent, 0, 2)
        total = kept + other.astype(jnp.float32)
        return (total + bias).astype(jnp.bfloat16), before

    half = core_sum(jnp.concatenate([merged, one], axis=1))
    near, _ = reduced(half[0], half[1])
    first = core_sum(two)[0]
    last = core_sum(three)[0]
    pair, near = reduced(first, last, near)
    pieces = [near, swap(near, 1, 2)]
    pieces += [swap(pair, 2, 0), swap(pair, 3, 2)]

    slot = jnp.right_shift(me, 1)
    row_count = lax.dynamic_index_in_dim(mine, slot, 0, keepdims=False)
    first_row = jnp.bitwise_and(me, 1) * (rows // 2)
    live_rows = jnp.right_shift(row_count, 2) - first_row
    return place((rank, live_rows), pieces, block_width)


def solution(mesh):
    return jax.shard_map(
        compute,
        mesh=mesh,
        in_specs=(
            P("dp", "tensor"),
            P(),
            P(),
            P(),
            P(None, None, "tensor"),
            P(None, "tensor"),
            P(None, "tensor"),
            P("tensor"),
            P("tensor"),
            P("tensor"),
            P(None, "tensor", "dp"),
            P(),
        ),
        out_specs=P(("dp", "tensor"), None),
        check_vma=False,
    )
```
